32 devices in a mesh: dp: 8 (over z, core), tensor: 4 (over y, x).
Axes of the slice: x: 2, y: 2, z: 4, core: 2. Of those that a mesh axis runs over, the one named last changes fastest.
Arguments:
- tokens: bfloat16 [1024, 2048], P(('dp', 'tensor')), may hold values from -6 to 6
- gate_weight: bfloat16 [2048, 8192], P(None, 'tensor'), may hold values from -0.125 to 0.125
- up_act: bfloat16 [1024, 8192], P('dp', 'tensor'), may hold values from -6 to 6
- cotangent: bfloat16 [1024, 8192], P('dp', 'tensor'), may hold values from -6 to 6
- moment1: bfloat16 [2048, 8192], P('dp', 'tensor'), may hold values from -0.359375 to 0.359375
- moment2: bfloat16 [2048, 8192], P('dp', 'tensor'), may hold values from 0.0039978027 to 0.039794922
Outputs:
- in_grad: bfloat16 [1024, 2048], P(('dp', 'tensor'))
- up_grad: bfloat16 [1024, 8192], P('dp', 'tensor')
- new_moment1: bfloat16 [2048, 8192], P('dp', 'tensor')
- new_moment2: bfloat16 [2048, 8192], P('dp', 'tensor')
- update: float32 [2048, 8192], P('dp', 'tensor')
The draws below stay inside these ranges and needn't reach their ends.
All inputs are finite; a program needn't handle non-finite values.
Results may differ from the reference program's by a relative error of at most 0.015.
Values may be sent and summed in bfloat16 or wider, within the bound.
No kernel may reach another device: no remote copies, remote signals or barrier semaphores. Data moves between devices by JAX's collectives and lax.ppermute only.
A program may use at most 64 MiB of HBM per device.

```python
import math
import jax
import jax.numpy as jnp
from jax import lax

DW = 2048
FFW = 8192
GROUP = 128
REPLICAS = 8
TENSOR_WAYS = 4
TOKENS = 1024


def strengthened(array, own_key, source, target, parts, factor):
    def block_of(axis_at):
        return (jnp.arange(array.shape[axis_at]) // (array.shape[axis_at] // parts)).reshape((-1,) + (1,) * (array.ndim - 1 - axis_at))

    one_side = jax.random.permutation(own_key, parts)[block_of(target)]
    second = (block_of(target) + parts // 2) % parts
    return jnp.where((block_of(source) == one_side) | (block_of(source) == second), factor * array, array)


def block_levels(rng, shape, cuts, smallest, high):
    def one(position, blocks):
        heights = jax.random.uniform(jax.random.fold_in(jax.random.fold_in(rng, 6), position), (blocks,), jnp.float32, smallest / len(cuts), high / len(cuts))
        return jnp.repeat(jnp.exp(heights), shape[position] // blocks).reshape((-1,) + (1,) * (len(shape) - position - 1))

    factor_of = one(*cuts[0])
    for cut in cuts[1:]:
        factor_of = factor_of * one(*cut)
    return factor_of


def gaussian(stream_key, dims, deviation, most, shards=(), dtype=jnp.bfloat16):
    drawn = jax.random.normal(stream_key, dims, jnp.float32) * deviation
    if len(shards) > 0:
        drawn = block_levels(stream_key, dims, shards, -0.22, 0.18) * drawn
    return jnp.clip(drawn, min=-most, max=most).astype(dtype)


def gaussian_with(stream_key, shape, deviation, bound, shards, heavy, held_as=jnp.bfloat16):
    values = deviation * jax.random.normal(stream_key, shape, jnp.float32)
    if shards:
        values = values * block_levels(stream_key, shape, shards, -0.22, 0.18)
    return jnp.clip(strengthened(values, jax.random.fold_in(stream_key, 3), *heavy), -bound, bound).astype(held_as)


def setup_inputs(seed: int = 0) -> dict:
    keys = jax.random.split(jax.random.key(seed), 7)
    tokens = gaussian_with(keys[0], (TOKENS, DW), 1.0, 6.0, ((0, 32),), (0, 1, 32, 2.75))
    gate_weight = gaussian(keys[1], (DW, FFW), DW ** -0.5, 0.125, ((1, 4),))
    up_act = gaussian(keys[2], (TOKENS, FFW), 1.0, 6.0, ((0, 8), (1, 4)))
    cotangent = gaussian(keys[3], (TOKENS, FFW), 1.0, 6.0, ((0, 8), (1, 4)))
    moment1 = gaussian(keys[4], (DW, FFW), 0.06, 0.359375, ((0, 8), (1, 4)))
    moment2 = jnp.clip(jnp.exp(math.log(0.039794922) - 2.2979944 * jax.random.uniform(keys[5], (DW, FFW), jnp.float32) ** block_levels(keys[5], (DW, FFW), ((0, 8), (1, 4)), -0.2, 0.2)), 0.0039978027, 0.039794922).astype(jnp.bfloat16)
    return dict(tokens=tokens, gate_weight=gate_weight, up_act=up_act, cotangent=cotangent, moment1=moment1, moment2=moment2)


def reference(tokens, gate_weight, up_act, cotangent, moment1, moment2):
    hidden_cols = FFW // TENSOR_WAYS
    token_sets = tokens.reshape(REPLICAS, GROUP, DW)
    up_sets = up_act.reshape(REPLICAS, GROUP, FFW)
    cot_sets = cotangent.reshape(REPLICAS, GROUP, FFW)
    weight_blocks = gate_weight.astype(jnp.float32).reshape(DW, TENSOR_WAYS, hidden_cols)

    def replica(running, operands):
        feature_rows, up_rows, cot_rows = operands
        gate_pre = jnp.dot(feature_rows, gate_weight, preferred_element_type=jnp.float32)
        sigmoid_gate = jax.nn.sigmoid(gate_pre)
        cot_float = cot_rows.astype(jnp.float32)
        up_result = (cot_float * gate_pre * sigmoid_gate).astype(jnp.bfloat16)
        gate_grad = (cot_float * up_rows.astype(jnp.float32) * sigmoid_gate * (1.0 + gate_pre * (1.0 - sigmoid_gate))).astype(jnp.bfloat16)
        pieces = jnp.einsum('gkc,dkc->kgd', gate_grad.astype(jnp.float32).reshape(GROUP, TENSOR_WAYS, hidden_cols), weight_blocks)
        input_rows = lax.optimization_barrier(jnp.sum(pieces.astype(jnp.bfloat16).astype(jnp.float32), axis=0)).astype(jnp.bfloat16)
        partial_value = jnp.dot(feature_rows.T, gate_grad, preferred_element_type=jnp.float32).astype(jnp.bfloat16)
        return (running + partial_value.astype(jnp.float32), (input_rows, up_result))
    start_sum = jnp.zeros((DW, FFW), jnp.float32)
    grad_total, (input_sets, up_results) = lax.scan(replica, start_sum, (token_sets, up_sets, cot_sets))
    grad = grad_total * (1.0 / math.sqrt(REPLICAS * GROUP))
    first = 0.9 * moment1.astype(jnp.float32) + 0.1 * grad
    second = 0.95 * moment2.astype(jnp.float32) + 0.05 * grad * grad
    update = first / (jnp.sqrt(second) + 1e-08)
    return (input_sets.reshape(TOKENS, DW), up_results.reshape(TOKENS, FFW), first.astype(jnp.bfloat16), second.astype(jnp.bfloat16), update)
```

```python
import math

import jax
import jax.numpy as jnp
from jax import lax
from jax.sharding import PartitionSpec as P

CHUNKS = 4


def activation(tokens_all, gate_weight, up_act, cotangent):
    gate_pre = jnp.dot(tokens_all, gate_weight, preferred_element_type=jnp.float32)
    sig = jax.nn.sigmoid(gate_pre)
    cot = cotangent.astype(jnp.float32)
    up_grad = (cot * gate_pre * sig).astype(jnp.bfloat16)
    gate_grad = (cot * up_act.astype(jnp.float32) * sig * (1.0 + gate_pre * (1.0 - sig))).astype(
        jnp.bfloat16
    )
    return up_grad, gate_grad


def adam(grad, moment1, moment2):
    first = 0.9 * moment1.astype(jnp.float32) + 0.1 * grad
    second = 0.95 * moment2.astype(jnp.float32) + 0.05 * grad * grad
    update = first / (jnp.sqrt(second) + 1e-08)
    return first.astype(jnp.bfloat16), second.astype(jnp.bfloat16), update


def dot_nt(a, b):
    return lax.dot_general(a, b, (((1,), (1,)), ((), ())), preferred_element_type=jnp.float32)


def dot_tn(a, b):
    return lax.dot_general(a, b, (((0,), (0,)), ((), ())), preferred_element_type=jnp.float32)


def reduced(tokens, gate_weight, up_act, cotangent, moment1, moment2):
    gathered = lax.all_gather(tokens, "tensor", axis=0, tiled=True)
    up_grad, gate_grad = activation(gathered, gate_weight, up_act, cotangent)
    in_grad = lax.psum_scatter(
        dot_nt(gate_grad, gate_weight).astype(jnp.bfloat16), "tensor", scatter_dimension=0, tiled=True
    )
    partial_value = dot_tn(gathered, gate_grad).astype(jnp.bfloat16)
    grad_shard = lax.psum_scatter(
        partial_value.astype(jnp.float32), "dp", scatter_dimension=0, tiled=True
    )
    grad = grad_shard * (1.0 / math.sqrt(lax.axis_size("dp") * gathered.shape[0]))
    return (in_grad, up_grad, *adam(grad, moment1, moment2))


def swapped(value, axis, k):
    return lax.ppermute(value, axis, [(i, i ^ k) for i in range(lax.axis_size(axis))])


def ordered(slots, me):
    out = []
    for j in range(len(slots)):
        cand = [slots[j ^ w] for w in range(len(slots))]
        bit = 1
        while len(cand) > 1:
            odd = (me & bit) != 0
            cand = [jnp.where(odd, cand[i + 1], cand[i]) for i in range(0, len(cand), 2)]
            bit *= 2
        out.append(cand[0])
    return out


def gathered_over(value, axis):
    slots = [value] + [swapped(value, axis, k) for k in range(1, lax.axis_size(axis))]
    return ordered(slots, lax.axis_index(axis))


def exchanged(tokens, gate_weight, up_act, cotangent, moment1, moment2):
    n, ways = lax.axis_size("dp"), lax.axis_size("tensor")
    chips = n // 2
    at, way = lax.axis_index("dp"), lax.axis_index("tensor")
    chip, core = at // 2, at % 2
    few, width = tokens.shape
    owned = moment1.shape[0]
    pair = 2 * owned
    cols = gate_weight.shape[1]

    gathered = jnp.concatenate(gathered_over(tokens, "tensor"), axis=0)

    def shift(value, s):
        return lax.ppermute(value, "dp", [(i, (i + 2 * s) % n) for i in range(n)])

    far = []
    for s in range(1, chips):
        to = (chip + s) % chips
        far.append(shift(lax.dynamic_slice_in_dim(tokens, to * pair, pair, 1), s))
    far = gathered_over(jnp.concatenate(far, axis=0), "tensor")

    up_grad, gate_grad = activation(gathered, gate_weight, up_act, cotangent)

    step = cols // CHUNKS
    parts = [[gate_grad[:, j * step : (j + 1) * step]] for j in range(CHUNKS)]
    for s in range(1, chips):
        for part in parts:
            part.append(shift(part[-1], 1))

    term = dot_nt(gate_grad, gate_weight).astype(jnp.bfloat16)
    block = lambda w: lax.dynamic_slice_in_dim(term, w * few, few, 0)
    total = block(way).astype(jnp.float32)
    for k in range(1, ways):
        total = total + swapped(block(way ^ k), "tensor", k).astype(jnp.float32)
    in_grad = total.astype(jnp.bfloat16)

    def rows_of(which):
        mine = lax.dynamic_slice_in_dim(gathered, (2 * chip + which) * owned, owned, 1)
        rest = [lax.dynamic_slice_in_dim(f, which * owned, owned, 1) for f in far]
        out = [mine]
        for s in range(1, chips):
            out.append(jnp.concatenate([r[(s - 1) * few : s * few] for r in rest], axis=0))
        return out

    own_rows, other_rows = rows_of(core), rows_of(1 - core)

    def product(rows, part):
        head = dot_tn(jnp.concatenate(rows[:-1], axis=0), jnp.concatenate(part[:-1], axis=0))
        return head + dot_tn(rows[-1], part[-1])

    scale = 1.0 / math.sqrt(n * gathered.shape[0])
    results = []
    for j, part in enumerate(parts):
        other = swapped(product(other_rows, part).astype(jnp.bfloat16), "dp", 1)
        grad = (product(own_rows, part) + other.astype(jnp.float32)) * scale
        sel = slice(j * step, (j + 1) * step)
        results.append(adam(grad, moment1[:, sel], moment2[:, sel]))
    new = [jnp.concatenate(list(r), axis=1) for r in zip(*results)]
    return (in_grad, up_grad, *new)


def local(tokens, gate_weight, up_act, cotangent, moment1, moment2):
    n, ways = lax.axis_size("dp"), lax.axis_size("tensor")
    total_tokens = n * up_act.shape[0]
    lighter = total_tokens * 2 <= gate_weight.shape[0] * 4
    if lighter and n % 2 == 0 and ways & (ways - 1) == 0:
        return exchanged(tokens, gate_weight, up_act, cotangent, moment1, moment2)
    return reduced(tokens, gate_weight, up_act, cotangent, moment1, moment2)


def solution(mesh):
    placed = (
        P(("dp", "tensor"), None),
        P(None, "tensor"),
        P("dp", "tensor"),
        P("dp", "tensor"),
        P("dp", "tensor"),
        P("dp", "tensor"),
    )
    return jax.shard_map(
        local,
        mesh=mesh,
        in_specs=placed,
        out_specs=(
            P(("dp", "tensor"), None),
            P("dp", "tensor"),
            P("dp", "tensor"),
            P("dp", "tensor"),
            P("dp", "tensor"),
        ),
        check_vma=False,
    )
```
